32 devices in a mesh: seq: 8 (over z, x), chan: 4 (over y, core).
Axes of the slice: x: 2, y: 2, z: 4, core: 2. Of those that a mesh axis runs over, the one named last changes fastest.
Arguments:
- x_in: bfloat16 [6144, 5120], P('seq', 'chan'), may hold values from -120 to 120
- z_gate: bfloat16 [6144, 5120], P('seq', 'chan'), may hold values from -6 to 6
- b_proj: bfloat16 [6144, 128], P('seq'), may hold values from -6 to 6
- c_proj: bfloat16 [6144, 128], P('seq'), may hold values from -6 to 6
- dt_step: float32 [80, 6144], P('chan', 'seq'), may hold values from 0 to 1
- a_log: float32 [80], P('chan'), may hold values from -0.35 to 0.35
- skip_gain: float32 [80], P('chan'), may hold values from 0.5 to 1.5
- norm_gain: float32 [5120], P('chan'), may hold values from 0.5 to 1.5
- out_weight: bfloat16 [2560, 5120], P('seq', 'chan'), may hold values from -0.078125 to 0.078125
- out_grad: bfloat16 [6144, 2560], P('seq'), may hold values from -6 to 6
Outputs:
- d_x: bfloat16 [6144, 5120], P('seq', 'chan')
- d_z: bfloat16 [6144, 5120], P('seq', 'chan')
- d_dt: float32 [80, 6144], P('chan', 'seq')
- d_out_weight: float32 [2560, 5120], P('seq', 'chan')
The draws below stay inside these ranges and needn't reach their ends.
All inputs are finite; a program needn't handle non-finite values.
Results may differ from the reference program's by a relative error of at most 0.005.
Values may be sent and summed in bfloat16 or wider, within the bound.
A program may use at most 128 MiB of HBM per device.

```python
import math
from functools import partial
import jax
import jax.numpy as jnp
from jax import lax

D = 2560
SCAN_HEADS = 80
STATE = 128
GROUP = 256
TOK_DEV = 768
E = 5120
SEQUENCE_TOKENS = 6144


def draw_x_in(key, part):
    random_keys = jax.random.split(key, 3)
    channel = jnp.arange(E, dtype=jnp.float32) / E
    random_part = jnp.clip(jax.random.normal(random_keys[0], (SEQUENCE_TOKENS, E), jnp.float32), -6.0, 6.0)
    row_scale = jnp.exp(jax.random.uniform(random_keys[1], (SEQUENCE_TOKENS, 1), jnp.float32, math.log(0.3), math.log(3.0)))
    col_scale = jnp.exp(jax.random.uniform(random_keys[2], (1, E), jnp.float32, math.log(0.3), math.log(3.0))) * 1.7320508 ** channel[None, :]
    value_entries = random_part * row_scale * col_scale
    return value_entries.astype(jnp.bfloat16)


def draw_dt_step(key, part):
    random_keys = jax.random.split(key, 7)
    blocks = SEQUENCE_TOKENS // TOK_DEV
    slow_head = jax.random.uniform(random_keys[0], (SCAN_HEADS, 1), jnp.float32) < 0.5
    fast_rate = 7.0 / GROUP * jnp.exp(jax.random.uniform(random_keys[1], (SCAN_HEADS, 1), jnp.float32, math.log(0.75), math.log(1.15)))
    slow_rate = jnp.exp(jax.random.uniform(random_keys[2], (SCAN_HEADS, 1), jnp.float32, math.log(0.2), math.log(0.6))) / SEQUENCE_TOKENS
    base_rate = jnp.where(slow_head, slow_rate, fast_rate)
    device_factor = jnp.exp(jax.random.uniform(random_keys[3], (SCAN_HEADS, blocks), jnp.float32, math.log(0.5), math.log(2.0)))
    spread = jnp.repeat(device_factor, TOK_DEV, axis=1)
    jitter = jnp.exp(jax.random.uniform(random_keys[4], (SCAN_HEADS, SEQUENCE_TOKENS), jnp.float32, math.log(0.5), math.log(2.0)))
    value_entries = base_rate * spread * jitter
    spike_start = jax.random.randint(random_keys[5], (SCAN_HEADS, 2), 0, SEQUENCE_TOKENS)
    spike_length = jax.random.uniform(random_keys[6], (SCAN_HEADS, 2), jnp.float32, 0.25, 0.5)
    token_places = jnp.arange(SEQUENCE_TOKENS, dtype=jnp.int32)
    found_pairs = token_places[None, :, None] == spike_start[:, None, :]
    spike_list = jnp.max(jnp.where(found_pairs, spike_length[:, None, :], 0.0), axis=2)
    return jnp.maximum(value_entries, spike_list).astype(jnp.float32)


def strengthened(drawn, stream_key, source, target, blocks, factor):
    owner, partner = [(jnp.arange(drawn.shape[axis_at]) // (drawn.shape[axis_at] // blocks)).reshape([-1 if axis == axis_at else 1 for axis in range(drawn.ndim)]) for axis_at in (source, target)]
    chosen = jax.random.permutation(stream_key, blocks)[partner]
    strong = (owner == chosen) | (owner == (partner + blocks // 2) % blocks)
    return jnp.where(strong, factor * drawn, drawn)


def shard_levels(key, shape, cuts, least, largest):
    def one(dim, parts):
        steps = jax.random.uniform(jax.random.fold_in(jax.random.fold_in(key, 6), dim), (parts,), jnp.float32, least / len(cuts), largest / len(cuts))
        return jnp.repeat(jnp.exp(steps), shape[dim] // parts).reshape((-1,) + (1,) * (len(shape) - dim - 1))

    gain = one(*cuts[0])
    for cut in cuts[1:]:
        gain = gain * one(*cut)
    return gain


def bell_draw(key, dims, deviation, most, shards=(), kind=jnp.bfloat16):
    entries = deviation * jax.random.normal(key, dims, jnp.float32)
    if shards:
        entries = entries * shard_levels(key, dims, shards, -0.22, 0.18)
    return jnp.clip(entries, -most, most).astype(kind)


def gaussian_with(rng, dims, scale, most, shards, heavy, held_as=jnp.bfloat16):
    drawn = scale * jax.random.normal(rng, dims, jnp.float32)
    if shards:
        drawn = drawn * shard_levels(rng, dims, shards, -0.22, 0.18)
    return jnp.clip(strengthened(drawn, jax.random.fold_in(rng, 3), *heavy), -most, most).astype(held_as)


def setup_inputs(seed: int = 0) -> dict:
    arg_keys = jax.random.split(jax.random.key(seed), 11)
    return {
        "x_in": draw_x_in(jax.random.fold_in(arg_keys[10], 71), 0),
        "z_gate": bell_draw(arg_keys[1], (SEQUENCE_TOKENS, E), 1.0, 6.0, ((0, 8), (1, 4))),
        "b_proj": bell_draw(arg_keys[2], (SEQUENCE_TOKENS, STATE), 1.0, 6.0, ((0, 8),)),
        "c_proj": bell_draw(arg_keys[3], (SEQUENCE_TOKENS, STATE), 1.0, 6.0, ((0, 8),)),
        "dt_step": draw_dt_step(jax.random.fold_in(arg_keys[10], 71), 0),
        "a_log": jnp.clip(jax.random.uniform(arg_keys[5], (SCAN_HEADS,), jnp.float32, -0.35, 0.35) * shard_levels(arg_keys[5], (SCAN_HEADS,), ((0, 4),), -0.4, 0.0), -0.35, 0.35),
        "skip_gain": jnp.clip(1.0 + 0.1 * jax.random.normal(arg_keys[6], (SCAN_HEADS,), jnp.float32), 0.5, 1.5),
        "norm_gain": jnp.clip(1.0 + 0.1 * jax.random.normal(arg_keys[7], (E,), jnp.float32), 0.5, 1.5),
        "out_weight": bell_draw(arg_keys[8], (D, E), E ** -0.5, 0.078125, ((0, 8), (1, 4))),
        "out_grad": gaussian_with(arg_keys[9], (SEQUENCE_TOKENS, D), 1.0, 6.0, ((0, 8),), (0, 1, 8, 2.0)),
    }


norm_eps = 1e-05
highest = lax.Precision.HIGHEST

def group_step(state_in, pieces, decay_rates, skip_gain):
    x_part, dt_part, b_part, c_part = pieces
    log_decay = jnp.cumsum(-decay_rates[:, None] * dt_part, axis=1)
    length = dt_part.shape[1]
    row_ids = lax.broadcasted_iota(jnp.int32, (length, length), 0)
    col_ids = lax.broadcasted_iota(jnp.int32, (length, length), 1)
    causal = (row_ids >= col_ids)[None]
    log_gap = jnp.where(causal, log_decay[:, :, None] - log_decay[:, None, :], 0.0)
    decay_mat = jnp.where(causal, jnp.exp(log_gap), 0.0)
    affinity = jnp.dot(c_part, b_part.T, precision=highest)
    weighted = x_part * jnp.transpose(dt_part)[:, :, None]
    within = jnp.einsum('hts,shp->thp', decay_mat * affinity[None], weighted, precision=highest)
    carried = jnp.transpose(jnp.exp(log_decay))[:, :, None] * jnp.einsum('tn,hpn->thp', c_part, state_in, precision=highest)
    output = within + carried + skip_gain[None, :, None] * x_part
    to_end = jnp.exp(log_decay[:, -1:] - log_decay)
    update = jnp.einsum('shp,hs,sn->hpn', weighted, to_end, b_part, precision=highest)
    state_out = jnp.exp(log_decay[:, -1])[:, None, None] * state_in + update
    return (state_out, output)

def ssd_local(x_vals, dt_vals, b_vals, c_vals, decay_rates, skip_gain, state_in):
    length, head_count, head_size = x_vals.shape
    blocks = length // GROUP
    x_blocks = x_vals.reshape(blocks, GROUP, head_count, head_size)
    dt_blocks = jnp.transpose(dt_vals.reshape(head_count, blocks, GROUP), (1, 0, 2))
    b_blocks = b_vals.reshape(blocks, GROUP, -1)
    c_blocks = c_vals.reshape(blocks, GROUP, -1)
    stepper = jax.checkpoint(partial(group_step, decay_rates=decay_rates, skip_gain=skip_gain))
    state_out, outputs = lax.scan(stepper, state_in, (x_blocks, dt_blocks, b_blocks, c_blocks))
    return (outputs.reshape(length, head_count, head_size), state_out)

def reference(x_in, z_gate, b_proj, c_proj, dt_step, a_log, skip_gain, norm_gain, out_weight, out_grad):
    total, width = x_in.shape
    head_count = a_log.shape[0]
    head_size = width // head_count
    decay_rates = jnp.exp(a_log)
    b_vals = b_proj.astype(jnp.float32)
    c_vals = c_proj.astype(jnp.float32)
    zero_state = jnp.zeros((head_count, head_size, b_vals.shape[1]), jnp.float32)

    def forward(x_arg, z_arg, dt_arg):
        x_vals = x_arg.astype(jnp.float32).reshape(total, head_count, head_size)
        y_vals, state_end = ssd_local(x_vals, dt_arg, b_vals, c_vals, decay_rates, skip_gain, zero_state)
        gated_y = y_vals.reshape(total, width) * jax.nn.silu(z_arg.astype(jnp.float32))
        scale_inv = lax.rsqrt(lax.optimization_barrier(jnp.mean(gated_y * gated_y, axis=1, keepdims=True)) + norm_eps)
        return (gated_y * scale_inv * norm_gain).astype(jnp.bfloat16)
    normed, pull_back = jax.vjp(forward, x_in, z_gate, dt_step)
    grad_norm = jnp.dot(out_grad, out_weight, preferred_element_type=jnp.float32).astype(jnp.bfloat16)
    weight_grad = lax.dot_general(out_grad, normed, (((0,), (0,)), ((), ())), preferred_element_type=jnp.float32)
    grad_x, grad_z, grad_dt = pull_back(grad_norm)
    return (grad_x, grad_z, grad_dt, weight_grad)
```

```python
from functools import partial

import jax
import jax.numpy as jnp
from jax import lax
from jax.experimental import pallas as pl
from jax.experimental.pallas import tpu as pltpu
from jax.sharding import PartitionSpec as P

CHUNK = 128
LANES = 128
norm_eps = 1e-05
highest = lax.Precision.HIGHEST
f32 = jnp.float32
bf16 = jnp.bfloat16


def mm(a, b, dims=((1,), (0,))):
    return lax.dot_general(a.astype(bf16), b.astype(bf16), (dims, ((), ())), preferred_element_type=f32)


def split(v):
    hi = v.astype(bf16)
    return hi, (v - hi.astype(f32)).astype(bf16)


def head_of(width, size):
    rows = lax.broadcasted_iota(jnp.int32, (LANES, width), 0)
    cols = lax.broadcasted_iota(jnp.int32, (LANES, width), 1)
    return jnp.where((cols >= rows * size) & (cols < (rows + 1) * size), 1.0, 0.0).astype(bf16)


def expand(v, select):
    hi, lo = split(v)
    return mm(jnp.concatenate([hi, lo], axis=1), jnp.concatenate([select, select], axis=0))


def per_head(v, select):
    hi, lo = split(v)
    return mm(hi, select, ((1,), (1,))) + mm(lo, select, ((1,), (1,)))


def run_sum(log_step):
    rows = lax.broadcasted_iota(jnp.int32, (CHUNK, CHUNK), 0)
    cols = lax.broadcasted_iota(jnp.int32, (CHUNK, CHUNK), 1)
    upper = jnp.where(rows <= cols, 1.0, 0.0)
    return jnp.dot(log_step, upper, precision=highest, preferred_element_type=f32)


def state_kernel(size, x_ref, b_ref, step_ref, dt_ref, out_ref):
    @pl.when(pl.program_id(0) == 0)
    def _():
        out_ref[...] = jnp.zeros_like(out_ref)

    select = head_of(x_ref.shape[1], size)
    log_row = run_sum(step_ref[...])
    last = log_row[:, CHUNK - 1 :]
    weight = jnp.transpose(jnp.exp(last - log_row) * dt_ref[...])
    whole = jnp.transpose(jnp.broadcast_to(jnp.exp(last), (LANES, CHUNK)))
    scaled = expand(weight, select) * x_ref[...].astype(f32)
    out_ref[...] = expand(whole[:8], select)[:1] * out_ref[...] + mm(b_ref[...], scaled, ((0,), (0,)))


def pair_decay(log_row, log_col, head):
    rows = lax.broadcasted_iota(jnp.int32, (CHUNK, CHUNK), 0)
    cols = lax.broadcasted_iota(jnp.int32, (CHUNK, CHUNK), 1)
    causal = rows >= cols
    parts = []
    for h in (head, head + 1):
        gap = log_col[:, h : h + 1] - log_row[h : h + 1, :]
        parts.append(jnp.where(causal, jnp.exp(jnp.where(causal, gap, 0.0)), 0.0))
    return parts


def forward_kernel(
    size, x_ref, z_ref, g_ref, b_ref, c_ref, step_ref, dt_ref, skip_ref, gain_ref, first_ref,
    y_ref, stat_ref, saved_ref, state_ref
):
    @pl.when(pl.program_id(0) == 0)
    def _():
        state_ref[...] = first_ref[...]

    width = x_ref.shape[1]
    select = head_of(width, size)
    log_row = run_sum(step_ref[...])
    log_col = jnp.transpose(log_row)
    last = log_row[:, CHUNK - 1 :]
    dt_row = dt_ref[...]
    weight = jnp.transpose(jnp.exp(last - log_row) * dt_row)
    whole = jnp.transpose(jnp.broadcast_to(jnp.exp(last), (LANES, CHUNK)))
    x_vals = x_ref[...]
    x_wide = x_vals.astype(f32)
    state = state_ref[...]
    saved_ref[0] = state.astype(bf16)
    affinity = mm(c_ref[...], b_ref[...], ((1,), (1,)))
    base = expand(jnp.exp(log_col), select) * mm(c_ref[...], state) + skip_ref[...] * x_wide
    lane = lax.broadcasted_iota(jnp.int32, (CHUNK, 2 * size), 1)
    squares = jnp.zeros((CHUNK, 2 * size), f32)
    dots = jnp.zeros((CHUNK, 2 * size), f32)
    for pair in range(width // (2 * size)):
        at = slice(pair * 2 * size, (pair + 1) * 2 * size)
        mats = pair_decay(log_row, log_col, 2 * pair)
        mats = [
            (m * affinity * dt_row[2 * pair + i : 2 * pair + i + 1, :]).astype(bf16)
            for i, m in enumerate(mats)
        ]
        xp = x_vals[:, at]
        zero = jnp.zeros_like(xp)
        stacked = jnp.concatenate([jnp.where(lane < size, xp, zero), jnp.where(lane < size, zero, xp)], axis=0)
        y_pair = base[:, at] + mm(jnp.concatenate(mats, axis=1), stacked)
        y_ref[:, at] = y_pair
        z_pair = z_ref[:, at].astype(f32)
        gated = y_pair * z_pair / (1.0 + jnp.exp(-z_pair))
        squares += gated * gated
        dots += gated * g_ref[:, at].astype(f32) * gain_ref[:, at]
    stat_ref[:, 0:1] = jnp.sum(squares, axis=1, keepdims=True)
    stat_ref[:, 1:2] = jnp.sum(dots, axis=1, keepdims=True)
    scaled = expand(weight, select) * x_wide
    state_ref[...] = expand(whole[:8], select)[:1] * state + mm(b_ref[...], scaled, ((0,), (0,)))


def gate_kernel(
    size, y_ref, z_ref, g_ref, c_ref, step_ref, gain_ref, scale_ref, normed_ref, dy_ref, dz_ref, out_ref
):
    @pl.when(pl.program_id(0) == 0)
    def _():
        out_ref[...] = jnp.zeros_like(out_ref)

    select = head_of(y_ref.shape[1], size)
    inverse = scale_ref[:, 0:1]
    pull = scale_ref[:, 1:2]
    y_vals = y_ref[...]
    z_vals = z_ref[...].astype(f32)
    sig = 1.0 / (1.0 + jnp.exp(-z_vals))
    act = z_vals * sig
    gated = y_vals * act
    gain = gain_ref[...]
    normed_ref[...] = (gated * inverse * gain).astype(bf16)
    grad = inverse * (g_ref[...].astype(f32) * gain) - gated * pull
    dz_ref[...] = (grad * y_vals * sig * (1.0 + z_vals * (1.0 - sig))).astype(bf16)
    dy = grad * act
    dy_ref[...] = dy.astype(bf16)
    log_row = run_sum(step_ref[...])
    growth = jnp.transpose(jnp.exp(log_row))
    out_ref[...] = expand(growth[CHUNK - 8 :], select)[7:8] * out_ref[...] + mm(
        c_ref[...], expand(growth, select) * dy, ((0,), (0,))
    )


def backward_kernel(
    size, x_ref, dy_ref, b_ref, c_ref, step_ref, dt_ref, rate_ref, skip_ref, saved_ref, end_ref,
    dx_ref, ddt_ref, grad_ref, row_ref, col_ref
):
    @pl.when(pl.program_id(0) == 0)
    def _():
        grad_ref[...] = end_ref[...]
        row_ref[...] = jnp.zeros_like(row_ref)
        col_ref[...] = jnp.zeros_like(col_ref)

    width = x_ref.shape[1]
    select = head_of(width, size)
    log_row = run_sum(step_ref[...])
    log_col = jnp.transpose(log_row)
    last = log_row[:, CHUNK - 1 :]
    dt_row = dt_ref[...]
    to_end = jnp.exp(last - log_row)
    grad = grad_ref[...]
    saved = saved_ref[0]
    x_vals = x_ref[...]
    x_wide = x_vals.astype(f32)
    dy_vals = dy_ref[...]
    dy_wide = dy_vals.astype(f32)
    affinity = mm(c_ref[...], b_ref[...], ((1,), (1,)))
    from_end = mm(b_ref[...], grad)
    growth = jnp.exp(log_col)
    grown = expand(growth, select) * dy_wide
    carried = jnp.transpose(per_head(grown * mm(c_ref[...], saved), select))
    inner = jnp.transpose(per_head(x_wide * from_end, select)) * to_end
    product = jnp.sum(saved.astype(f32) * grad, axis=0, keepdims=True)
    product = jnp.transpose(per_head(jnp.broadcast_to(product, (LANES, width)), select))[:, :1]
    dxw = expand(jnp.transpose(to_end), select) * from_end
    dt_wide = expand(jnp.transpose(dt_row), select)
    skip_dy = skip_ref[...] * dy_wide
    lane = lax.broadcasted_iota(jnp.int32, (CHUNK, 2 * size), 1)
    for pair in range(width // (2 * size)):
        at = slice(pair * 2 * size, (pair + 1) * 2 * size)
        mats = [m * affinity for m in pair_decay(log_row, log_col, 2 * pair)]
        xp = x_vals[:, at]
        dyp = dy_vals[:, at]
        zero = jnp.zeros_like(xp)
        stacked = jnp.concatenate([jnp.where(lane < size, xp, zero), jnp.where(lane < size, zero, xp)], axis=0)
        prods = mm(dyp, stacked, ((1,), (1,)))
        for i in range(2):
            h = 2 * pair + i
            both = mats[i] * prods[:, i * CHUNK : (i + 1) * CHUNK]
            row_ref[h : h + 1, :] = jnp.sum(both, axis=0, keepdims=True)
            col_ref[:, h : h + 1] = jnp.sum(both * dt_row[h : h + 1, :], axis=1, keepdims=True)
        inside = mm(jnp.concatenate([m.astype(bf16) for m in mats], axis=1), dyp, ((0,), (0,)))
        inside = jnp.where(lane < size, inside[:CHUNK], inside[CHUNK:])
        dx_ref[:, at] = (dt_wide[:, at] * (dxw[:, at] + inside) + skip_dy[:, at]).astype(bf16)
    direct = row_ref[...]
    update = dt_row * inner
    d_log = jnp.transpose(col_ref[...]) - dt_row * direct + carried - update
    at_end = jnp.sum(update, axis=1, keepdims=True) + jnp.exp(last) * product
    rows = lax.broadcasted_iota(jnp.int32, (CHUNK, CHUNK), 0)
    cols = lax.broadcasted_iota(jnp.int32, (CHUNK, CHUNK), 1)
    lower = jnp.where(rows >= cols, 1.0, 0.0)
    later = jnp.dot(d_log, lower, precision=highest, preferred_element_type=f32) + at_end
    ddt_ref[...] = direct + inner - rate_ref[...] * later
    grad_ref[...] = expand(growth[CHUNK - 8 :], select)[7:8] * grad + mm(c_ref[...], grown, ((0,), (0,)))


def shards(
    x_in, z_gate, b_proj, c_proj, dt_step, a_log, skip_gain, norm_gain, out_weight, out_grad
):
    length, width = x_in.shape
    heads = a_log.shape[0]
    size = width // heads
    states = b_proj.shape[1]
    blocks = length // CHUNK
    peers, index = lax.axis_size("seq"), lax.axis_index("seq")

    def tok(w, rev=False):
        return pl.BlockSpec((CHUNK, w), lambda i: (blocks - 1 - i, 0) if rev else (i, 0))

    def row(rev=False):
        return pl.BlockSpec((LANES, CHUNK), lambda i: (0, blocks - 1 - i) if rev else (0, i))

    def all_of(r, w):
        return pl.BlockSpec((r, w), lambda i: (0, 0))

    def saved_at(rev=False):
        return pl.BlockSpec((1, states, width), lambda i: (blocks - 1 - i, 0, 0) if rev else (i, 0, 0))

    def shape(s, d):
        return jax.ShapeDtypeStruct(s, d)

    def call(kernel, name, ins, outs, out_shape, scratch=(), flops=10**9, moved=8 * 10**6):
        return pl.pallas_call(
            partial(kernel, size),
            grid=(blocks,),
            in_specs=ins,
            out_specs=outs,
            out_shape=out_shape,
            scratch_shapes=scratch,
            name=name,
            compiler_params=pltpu.CompilerParams(
                dimension_semantics=("arbitrary",), vmem_limit_bytes=48 * 1024 * 1024
            ),
            cost_estimate=pl.CostEstimate(flops=flops, bytes_accessed=moved, transcendentals=0),
        )

    weight_all = lax.all_gather(out_weight, "seq", axis=0, tiled=True)
    rates = jnp.exp(a_log)
    pad = ((0, LANES - heads), (0, 0))
    total = jnp.sum(-rates[:, None] * dt_step, axis=1)
    totals = lax.all_gather(total, "seq")
    dt_rows = jnp.pad(dt_step, pad)
    steps = jnp.pad(-rates[:, None] * dt_step, pad)
    rate_col = jnp.pad(rates[:, None], pad)
    skip = jnp.repeat(skip_gain, size)[None, :]
    gain = norm_gain[None, :]
    state_shape = shape((states, width), f32)
    full = all_of(states, width)

    local_state = call(
        state_kernel, "local_state", [tok(width), tok(states), row(), row()], full, state_shape
    )(x_in, b_proj, steps, dt_rows)
    weight_all, local_state = lax.optimization_barrier((weight_all, local_state))
    order = jnp.arange(peers)

    def entering(local, reverse):
        everything = lax.all_gather(local.astype(bf16), "seq")
        between = order[:, None] < order[None, :] if not reverse else order[:, None] > order[None, :]
        past = order < index if not reverse else order > index
        inside = (between & past[None, :]).astype(f32)
        decay = jnp.exp(jnp.sum(inside[:, :, None] * totals[None], axis=1))
        coef = jnp.where(past[:, None], decay, 0.0)
        coef = jnp.repeat(coef, size, axis=1)[:, None, :]
        return jnp.sum(coef * everything.astype(f32), axis=0)

    state_in = entering(local_state, False)
    grad_norm = jnp.dot(out_grad, weight_all, preferred_element_type=f32).astype(bf16)
    y_vals, stats, saved = call(
        forward_kernel,
        "scan_forward",
        [tok(width), tok(width), tok(width), tok(states), tok(states), row(), row(),
         all_of(1, width), all_of(1, width), full],
        (tok(width), tok(2), saved_at()),
        (shape((length, width), f32), shape((length, 2), f32), shape((blocks, states, width), bf16)),
        [pltpu.VMEM((states, width), f32)],
    )(x_in, z_gate, grad_norm, b_proj, c_proj, steps, dt_rows, skip, gain, state_in)
    sums = lax.psum(jnp.transpose(stats), "chan")
    full_width = width * lax.axis_size("chan")
    inverse = lax.rsqrt(sums[0] / full_width + norm_eps)
    scales = jnp.stack([inverse, inverse**3 * sums[1] / full_width], axis=1)
    normed, grad_y, grad_z, local_grad = call(
        gate_kernel,
        "gate_backward",
        [tok(width, True), tok(width, True), tok(width, True), tok(states, True), row(True),
         all_of(1, width), tok(2, True)],
        (tok(width, True), tok(width, True), tok(width, True), full),
        (shape((length, width), bf16),) * 3 + (state_shape,),
    )(y_vals, z_gate, grad_norm, c_proj, steps, gain, scales)
    grad_end = entering(local_grad, True)
    partial_weight = lax.dot_general(
        out_grad, normed, (((0,), (0,)), ((), ())), preferred_element_type=f32
    )
    weight_grad = reduce_rows(partial_weight, peers)
    grad_x, grad_dt = call(
        backward_kernel,
        "scan_backward",
        [tok(width, True), tok(width, True), tok(states, True), tok(states, True), row(True), row(True),
         all_of(LANES, 1), all_of(1, width), saved_at(True), full],
        (tok(width, True), row(True)),
        (shape((length, width), bf16), shape((LANES, length), f32)),
        [pltpu.VMEM((states, width), f32), pltpu.VMEM((LANES, CHUNK), f32), pltpu.VMEM((CHUNK, LANES), f32)],
    )(x_in, grad_y, b_proj, c_proj, steps, dt_rows, rate_col, skip, saved, grad_end)
    return (grad_x, grad_z, grad_dt[:heads], weight_grad)


def reduce_rows(value, peers):
    rows, width = value.shape
    parts = value.astype(bf16).reshape(peers, rows // peers, width)
    parts = lax.all_to_all(parts, "seq", 0, 0)
    return jnp.sum(parts.astype(f32), axis=0)


def solution(mesh):
    placed = (
        P("seq", "chan"),
        P("seq", "chan"),
        P("seq", None),
        P("seq", None),
        P("chan", "seq"),
        P("chan"),
        P("chan"),
        P("chan"),
        P("seq", "chan"),
        P("seq", None),
    )
    return jax.shard_map(
        shards,
        mesh=mesh,
        in_specs=placed,
        out_specs=(P("seq", "chan"), P("seq", "chan"), P("chan", "seq"), P("seq", "chan")),
        check_vma=False,
    )
```
